128 devices in a mesh: row: 32 (over z_hi, x, y), col: 4 (over z_lo, core).
Axes of the slice: x: 4, y: 4, z: 4 (z_hi: 2, z_lo: 2; z = z_hi * 2 + z_lo), core: 2. Of those that a mesh axis runs over, the one named last changes fastest.
Arguments:
- tokens: bfloat16 [1024, 8192], P('row', 'col'), may hold values from -6 to 6
- gate_codes: int32 [1024, 28672], P('col', 'row'), may hold values from -2147483648 to 2147483646
- up_codes: int32 [1024, 28672], P('col', 'row'), may hold values from -2147483648 to 2147483646
- down_codes: int32 [3584, 8192], P('row', 'col'), may hold values from -2147483648 to 2147483646
- gate_scales: bfloat16 [64, 28672], P('row'), may hold values from 0.0009994507 to 0.0049743652
- up_scales: bfloat16 [64, 28672], P('row'), may hold values from 0.0009994507 to 0.0049743652
- down_scales: bfloat16 [8192, 224], P('row'), may hold values from 0.00059890747 to 0.0029907227
Outputs:
- mixed: bfloat16 [1024, 8192], P('row', 'col')
The draws below stay inside these ranges and needn't reach their ends.
Inputs may be any that keep to these rules, and one draw needn't show every extreme that they name: Every word of gate_codes, up_codes and down_codes is an arbitrary 32-bit pattern: all sixteen codes occur in every nibble position.
All inputs are finite; a program needn't handle non-finite values.
Results may differ from the reference program's by a relative error of at most 0.025.
Values may be sent and summed in bfloat16 or wider, within the bound.
A program may use at most 128 MiB of HBM per device.

```python
import math
import jax
import jax.numpy as jnp
from jax import lax

D = 8192
FF = 28672
GROUP = 128
TOKENS = 1024
N_ROW = 32


def plant(drawn, rng, smallest, high):
    index_at = [jax.random.randint(jax.random.fold_in(rng, axis), (), 0, length) for axis, length in enumerate(drawn.shape)]
    main_axis = drawn.shape.index(max(drawn.shape))
    neighbour = index_at[:main_axis] + [(index_at[main_axis] + 1) % drawn.shape[main_axis]] + index_at[main_axis + 1:]
    return drawn.at[tuple(index_at)].set(smallest).at[tuple(neighbour)].set(high)


def level_of(rng, dims, pieces, least, high):
    def one(dim, blocks):
        draws = jax.random.uniform(jax.random.fold_in(jax.random.fold_in(rng, 6), dim), (blocks,), jnp.float32, least / len(pieces), high / len(pieces))
        return jnp.repeat(jnp.exp(draws), dims[dim] // blocks).reshape((-1,) + (1,) * (len(dims) - dim - 1))

    gain = one(*pieces[0])
    for cut in pieces[1:]:
        gain = gain * one(*cut)
    return gain


def gaussian(rng, extent, deviation, bound, shards=(), held_as=jnp.bfloat16):
    result = jax.random.normal(rng, extent, jnp.float32) * deviation
    if len(shards) > 0:
        result = level_of(rng, extent, shards, -0.22, 0.18) * result
    return jnp.clip(result, min=-bound, max=bound).astype(held_as)


def setup_inputs(seed: int = 0) -> dict:
    streams_of = jax.random.split(jax.random.key(seed), 8)
    return {
        "tokens": gaussian(streams_of[0], (TOKENS, D), 1.0, 6.0, ((0, 32), (1, 4))),
        "gate_codes": plant(jax.random.randint(streams_of[1], (D // 8, FF), -2147483648, 2147483647), jax.random.fold_in(streams_of[1], 1), -2147483648, 2147483646).astype(jnp.int32),
        "up_codes": plant(jax.random.randint(streams_of[2], (D // 8, FF), -2147483648, 2147483647), jax.random.fold_in(streams_of[2], 1), -2147483648, 2147483646).astype(jnp.int32),
        "down_codes": plant(jax.random.randint(streams_of[3], (FF // 8, D), -2147483648, 2147483647), jax.random.fold_in(streams_of[3], 1), -2147483648, 2147483646).astype(jnp.int32),
        "gate_scales": jnp.clip(jnp.exp(math.log(0.0049743652) - 1.6048472 * jax.random.uniform(streams_of[4], (D // GROUP, FF), jnp.float32) ** level_of(streams_of[4], (D // GROUP, FF), ((0, 32),), -0.2, 0.2)), 0.0009994507, 0.0049743652).astype(jnp.bfloat16),
        "up_scales": jnp.clip(jnp.exp(math.log(0.0049743652) - 1.6048472 * jax.random.uniform(streams_of[5], (D // GROUP, FF), jnp.float32) ** level_of(streams_of[5], (D // GROUP, FF), ((0, 32),), -0.2, 0.2)), 0.0009994507, 0.0049743652).astype(jnp.bfloat16),
        "down_scales": jnp.clip(jnp.exp(math.log(0.0029907227) - 1.6081632 * jax.random.uniform(streams_of[6], (D, FF // GROUP), jnp.float32) ** level_of(streams_of[6], (D, FF // GROUP), ((0, 32),), -0.2, 0.2)), 0.00059890747, 0.0029907227).astype(jnp.bfloat16),
    }


def unpack_codes(packed):
    nibbles = [jnp.bitwise_and(jnp.right_shift(packed, 4 * offset), 15) for offset in range(8)]
    stacked = jnp.stack(nibbles, axis=1)
    return stacked.reshape(packed.shape[0] * 8, packed.shape[1]) - 8


def dequantize_rows(packed, scale_rows, group_size):
    values = unpack_codes(packed).astype(jnp.float32)
    columns = values.shape[1]
    shaped = values.reshape(scale_rows.shape[0], group_size, columns) * scale_rows.astype(jnp.float32)[:, None, :]
    return shaped.reshape(values.shape[0], columns).astype(jnp.bfloat16)


def split_cols(array):
    return array.reshape(array.shape[0], N_ROW, array.shape[1] // N_ROW).transpose(1, 0, 2)


def reference(tokens, gate_codes, up_codes, down_codes, gate_scales, up_scales, down_scales):
    down_blocks = down_codes.reshape(N_ROW, down_codes.shape[0] // N_ROW, D)

    def one_block(running, inputs):
        gate_packed, up_packed, gate_scale, up_scale, down_packed, down_scale = inputs
        gate_sum = jnp.dot(tokens, dequantize_rows(gate_packed, gate_scale, GROUP), preferred_element_type=jnp.float32)
        up_sum = jnp.dot(tokens, dequantize_rows(up_packed, up_scale, GROUP), preferred_element_type=jnp.float32)
        hidden = (jax.nn.silu(gate_sum) * up_sum).astype(jnp.bfloat16)
        partial_value = jnp.dot(hidden, dequantize_rows(down_packed, down_scale.T, GROUP), preferred_element_type=jnp.float32).astype(jnp.bfloat16)
        return running + partial_value.astype(jnp.float32), None

    start_sum = jnp.zeros((tokens.shape[0], D), jnp.float32)
    running, unused = lax.scan(one_block, start_sum, (split_cols(gate_codes), split_cols(up_codes), split_cols(gate_scales), split_cols(up_scales), down_blocks, split_cols(down_scales)))
    return running.astype(jnp.bfloat16)
```

```python
import jax
import jax.numpy as jnp
from jax import lax
from jax.experimental import pallas as pl
from jax.experimental.pallas import tpu as pltpu
from jax.sharding import PartitionSpec as P

MESH = pl.DeviceIdType.MESH
BF, F32, I32 = jnp.bfloat16, jnp.float32, jnp.int32
SLOT = ((0, None, 5, None), (1, None, 4, None))
SIDES = ((7, 6), (2, 3))


def unit(w, line, p):
    if line in (1, 3):
        return SIDES[w][p // 2], p % 2 + (2 if line == 3 else 0)
    return SLOT[w][line], p


NCHUNK = 8
ALL = (0, 1, 2, 3)
LO, HI = pl.ds(0, 1024), pl.ds(1024, 1024)


def kernel(
    tok, gcode, ucode, dcode, gscale, uscale, dscale, out,
    x, o, w1, w2, gc, uc, dc, tk, gsv, usv, dsv, dt, ds, sg, su, sgf, suf, sd,
    pb, r1, s2, r2, hid, ra, rb, pa, pg, pd, rz,
    load_sem, sc_s, sc_r, ag_s, ag_r, agz_r, ch_s, c1_r, z1_r, z2_r, c2_r, rs_s, ra_r, rb_r, pa_r, pg_r, pd_r, rsz_r,
):
    row, col = lax.axis_index("row"), lax.axis_index("col")
    zhi, rem16 = row // 16, row % 16
    xx, yy = rem16 // 4, rem16 % 4
    core, zlo = col % 2, col // 2

    def at(zz, a, b):
        return (zz * 16 + a * 4 + b, col)

    xp, xm = at(zhi, (xx + 1) % 4, yy), at(zhi, (xx + 3) % 4, yy)
    yp, ym = at(zhi, xx, (yy + 1) % 4), at(zhi, xx, (yy + 3) % 4)
    zpart = at(1 - zhi, xx, yy)
    lpart = (row, (1 - zlo) * 2 + core)
    cpart = (row, zlo * 2 + 1 - core)
    nb = (((xp, xm), (yp, ym)), ((yp, ym), (xp, xm)))
    oz = 1 - zhi
    zxp, zxm = at(oz, (xx + 1) % 4, yy), at(oz, (xx + 3) % 4, yy)
    zyp, zym = at(oz, xx, (yy + 1) % 4), at(oz, xx, (yy + 3) % 4)
    passed = (((yp, ym), (xp, xm)), ((zyp, zym), (zxp, zxm)))

    def rcopy(src, dst, ss, rs, dev):
        return pltpu.make_async_remote_copy(
            src_ref=src, dst_ref=dst, send_sem=ss, recv_sem=rs,
            device_id=dev, device_id_type=MESH,
        )

    l_tok = pltpu.make_async_copy(tok, tk, load_sem.at[0])
    l_dsv = pltpu.make_async_copy(dscale, dsv, load_sem.at[1])
    l_g = pltpu.make_async_copy(gcode, gc, load_sem.at[2])
    l_u = pltpu.make_async_copy(ucode, uc, load_sem.at[3])
    l_d = pltpu.make_async_copy(dcode, dc, load_sem.at[4])
    l_gs = pltpu.make_async_copy(gscale, gsv, load_sem.at[5])
    l_us = pltpu.make_async_copy(uscale, usv, load_sem.at[6])
    for c in (l_tok, l_dsv, l_gs, l_us, l_g, l_u, l_d):
        c.start()

    barrier = pltpu.get_barrier_semaphore()
    for dev in (xp, xm, yp, ym, zpart, lpart, cpart, zxp, zxm, zyp, zym):
        pl.semaphore_signal(barrier, inc=1, device_id=dev, device_id_type=MESH)
    for k in range(8):
        src_row = col * 8 + k
        src_core = (k // 4 + (col % 2) * 2) // 2
        src_core = (src_core + 1 + yy + k % 4) % 2
        pl.semaphore_signal(barrier, inc=1, device_id=(src_row, zhi * 2 + src_core), device_id_type=MESH)

    ri = lax.broadcasted_iota(I32, (128, 128), 0)
    ci = lax.broadcasted_iota(I32, (128, 128), 1)
    perm = (ri == 8 * (ci & 15) + (ci >> 4)).astype(F32).astype(BF)

    def permuted(v):
        rows, cols = v.shape
        n = cols // 128
        tall = jnp.concatenate([v[:, b * 128 : (b + 1) * 128] for b in range(n)], axis=0)
        res = jnp.dot(tall, perm, preferred_element_type=F32).astype(BF)
        return [res[b * rows : (b + 1) * rows] for b in range(n)]

    l_tok.wait()
    for b, piece in enumerate(permuted(tk[...])):
        for h in range(2):
            x[0, h, 0, :, b * 128 : (b + 1) * 128] = piece[h * 16 : (h + 1) * 16]

    l_dsv.wait()
    dt[224:232, :] = jnp.zeros((8, 256), F32)
    dt[0:224, :] = dsv[...].astype(F32)
    for r in range(32):
        ds[r] = dt[7 * r : 7 * r + 8, :]
    y_first = (yy + core + xx // 2 + 1) % 2
    l_gs.wait()
    l_us.wait()

    pl.semaphore_wait(barrier, 19)

    def ag(w, h, ev, src, dst, dev):
        kind = 0 if ev < 2 or ev >= 16 else 1 if ev < 4 else 2 if ev < 12 else 3
        return rcopy(src, dst, ag_s.at[kind], ag_r.at[w, h, ev], dev)

    def ag_p1(first):
        def copies(w, h):
            s = SLOT[w][0]
            plus, minus = nb[h][0]
            a, b = (LO, HI) if first else (HI, LO)
            ev = 0 if first else 16
            return (
                ag(w, h, ev, x.at[s, h, 0, :, a], x.at[s, h, 1, :, a], minus),
                ag(w, h, ev + 1, x.at[s, h, 0, :, b], x.at[s, h, 3, :, b], plus),
            )

        return copies

    def ag_f1(w, h):
        s = SLOT[w][0]
        plus, minus = nb[h][0]
        lo, hi = pl.ds(0, 1024), pl.ds(1024, 1024)
        return (
            ag(w, h, 2, x.at[s, h, 1, :, lo], x.at[s, h, 2, :, lo], minus),
            ag(w, h, 3, x.at[s, h, 3, :, hi], x.at[s, h, 2, :, hi], plus),
        )

    def ag_p2(pos):
        def copies(w, h):
            plus, minus = nb[h][1]
            res = []
            for p in pos:
                own = x.at[SLOT[w][0], h, p]
                (a, i), (b, j) = unit(w, 1, p), unit(w, 3, p)
                res.append(ag(w, h, 4 + p, own, x.at[a, h, i], minus))
                res.append(ag(w, h, 8 + p, own, x.at[b, h, j], plus))
            return res

        return copies

    def ag_f2(pos):
        def copies(w, h):
            plus, minus = nb[h][1]
            res = []
            for p in pos:
                (a, i), dev = (unit(w, 1, p), minus) if p < 2 else (unit(w, 3, p), plus)
                res.append(ag(w, h, 12 + p, x.at[a, h, i], x.at[SLOT[w][2], h, p], dev))
            return res

        return copies

    def ag_z(h):
        return rcopy(x.at[SLOT[0][0], h, 0], x.at[SLOT[1][0], h, 0], ag_s.at[4], agz_r.at[h], zpart)

    def start(fn, w):
        for h in range(2):
            for c in fn(w, h):
                c.start()

    def arrived(fn, w):
        for h in range(2):
            for c in fn(w, h):
                c.wait_recv()

    start(ag_p1(True), 0)
    start(ag_p1(False), 0)
    for h in range(2):
        ag_z(h).start()

    k_me = row % 8
    scale_copies = []
    for j in range(8):
        dst_row = zlo * 16 + (j // 2) * 4 + (j % 2) * 2 + y_first
        dev = (dst_row, row // 8)
        cols = pl.ds(pl.multiple_of(dst_row * 896, 128), 896)
        dcols = pl.ds(pl.multiple_of(k_me * 256, 128), 256)
        scale_copies.append((
            rcopy(gsv.at[:, cols], sg.at[k_me], sc_s.at[0], sc_r.at[0], dev),
            rcopy(usv.at[:, cols], su.at[k_me], sc_s.at[1], sc_r.at[1], dev),
            rcopy(ds.at[dst_row], sd.at[pl.ds(0, 8), dcols], sc_s.at[2], sc_r.at[2], dev),
        ))
    for group in scale_copies:
        for c in group:
            c.start()
    start(ag_p2((0,)), 0)

    def all_of(ref, sem):
        pltpu.make_async_copy(ref, ref, sem).wait()

    def scale_arrived(kind):
        all_of((sg, su, sd)[kind].at[pl.ds(0, 8)], sc_r.at[kind])

    def unpack(codes, dst, groups, c0, n):
        def one(g, carry):
            w = codes[pl.ds(pl.multiple_of(g * 16, 16), 16), :] ^ jnp.int32(-2004318072)
            for k in range(8):
                v = lax.shift_right_arithmetic(lax.shift_left(w, jnp.int32(28 - 4 * k)), jnp.int32(28))
                dst[pl.ds(pl.multiple_of(g * 128 + k * 16, 16), 16), c0 : c0 + n] = v.astype(F32).astype(BF)
            return carry

        lax.fori_loop(0, groups, one, 0)

    def rescale(scale_rows, dst, groups, c0, n):
        def one(g, carry):
            s = scale_rows[pl.ds(g, 1), :].astype(BF)
            at = pl.ds(pl.multiple_of(g * 128, 128), 128)
            dst[at, c0 : c0 + n] = dst[at, c0 : c0 + n] * s
            return carry

        lax.fori_loop(0, groups, one, 0)

    l_g.wait()
    unpack(gc, w1, 16, 0, 896)
    l_u.wait()
    unpack(uc, w1, 16, 896, 896)
    arrived(ag_p1(True), 0)
    start(ag_f1, 0)
    def ev_z():
        for h in range(2):
            ag_z(h).wait_recv()
            for first in (True, False):
                for c in ag_p1(first)(1, h):
                    c.start()
            for c in ag_p2((0,))(1, h):
                c.start()

    def ev_rescale_down():
        l_d.wait()
        unpack(dc, w2, 7, 0, 2048)
        scale_arrived(2)
        rescale(sd, w2, 7, 0, 2048)

    def ev_p2(w, pos):
        arrived(ag_p2(pos), w)
        start(ag_f2(pos), w)

    def ev_f2(w):
        arrived(ag_f2(ALL), w)

    def ev_p1w1():
        arrived(ag_p1(True), 1)
        start(ag_f1, 1)
        arrived(ag_p1(False), 1)
        start(ag_p2((1, 3)), 1)

    def ev_f1w1():
        arrived(ag_f1, 1)
        start(ag_p2((2,)), 1)

    def ev_f1w0():
        arrived(ag_p1(False), 0)
        arrived(ag_f1, 0)

    ev_z()
    scale_arrived(0)
    scale_arrived(1)
    for k in range(8):
        sgf[2 * k : 2 * k + 2, :] = sg[k].astype(F32)
        suf[2 * k : 2 * k + 2, :] = su[k].astype(F32)
    rescale(sgf, w1, 16, 0, 896)
    rescale(suf, w1, 16, 896, 896)
    ev_f1w0()

    def c1(j):
        return rcopy(pb.at[j, 1 - core], r1.at[j], ch_s.at[0], c1_r.at[j], cpart)

    def z1(j):
        return rcopy(s2.at[j], r2.at[j], ch_s.at[1], z1_r.at[j], lpart)

    def z2(j):
        return rcopy(hid.at[j, core, zlo], hid.at[j, core, zlo], ch_s.at[2], z2_r.at[j], lpart)

    def c2(j):
        return rcopy(hid.at[j, core], hid.at[j, core], ch_s.at[3], c2_r.at[j], cpart)

    def st_g(j):
        p = jnp.dot(x[j].reshape(128, 2048), w1[...], preferred_element_type=F32)
        pb[j] = p.astype(BF).reshape(2, 2, 32, 1792)
        c1(j).start()

    def st_e1(j):
        c1(j).wait_recv()
        s2[j] = (pb[j, core, 1 - zlo].astype(F32) + r1[j, 1 - zlo].astype(F32)).astype(BF)
        z1(j).start()

    def st_e2(j):
        z1(j).wait_recv()
        tot = pb[j, core, zlo].astype(F32) + r1[j, zlo].astype(F32) + r2[j].astype(F32)
        gate, up = tot[:, :896], tot[:, 896:]
        hv = (gate / (1.0 + jnp.exp(-gate)) * up).astype(BF)
        for b, piece in enumerate(permuted(hv)):
            hid[j, core, zlo, :, b * 128 : (b + 1) * 128] = piece
        z2(j).start()

    def st_e3(j):
        z2(j).wait_recv()
        c2(j).start()

    def st_d(j):
        c2(j).wait_recv()
        r = jnp.dot(hid[j].reshape(128, 896), w2[...], preferred_element_type=F32)
        o[j] = r.astype(BF).reshape(2, 4, 16, 2048)

    def fsum(*vs):
        t = vs[0].astype(F32)
        for v in vs[1:]:
            t = t + v.astype(F32)
        return t.astype(BF)

    def rs_a(w, line, h):
        plus, minus = nb[h][0]
        n = 4 * w + line
        a, i = unit(w, line, 2)
        return (
            rcopy(o.at[a, h, i, :, LO], ra.at[n, h, 0], rs_s.at[0], ra_r.at[n, h, 0], plus),
            rcopy(o.at[a, h, i, :, HI], ra.at[n, h, 1], rs_s.at[0], ra_r.at[n, h, 1], minus),
        )

    def rs_b(w, line, h):
        plus, minus = nb[h][0]
        n = 4 * w + line
        (a, i), (b, k) = unit(w, line, 1), unit(w, line, 3)
        return (
            rcopy(o.at[a, h, i], rb.at[n, h, 0], rs_s.at[1], rb_r.at[n, h, 0], plus),
            rcopy(o.at[b, h, k], rb.at[n, h, 1], rs_s.at[1], rb_r.at[n, h, 1], minus),
        )

    def rs_c(w, h):
        far = SLOT[w][2]
        plus, minus = nb[h][1]
        return (
            rcopy(o.at[far, h, 0, :, LO], pa.at[w, h, 0], rs_s.at[2], pa_r.at[w, h, 0], plus),
            rcopy(o.at[far, h, 0, :, HI], pa.at[w, h, 1], rs_s.at[2], pa_r.at[w, h, 1], minus),
        )

    def rs_d(side):
        def copies(w, h):
            a, i = unit(w, 1 + 2 * side, 0)
            return (
                rcopy(o.at[a, h, i], pd.at[w, h, side], rs_s.at[3], pd_r.at[w, h, side], nb[h][1][side]),
            )

        return copies

    def rsz(h):
        return rcopy(o.at[SLOT[1][0], h, 0], rz.at[h], rs_s.at[4], rsz_r.at[h], zpart)

    def st_ra(w, line):
        for h in range(2):
            for c in rs_a(w, line, h):
                c.start()

    def st_rb(w, line):
        n = 4 * w + line
        (a, i), (b, k) = unit(w, line, 1), unit(w, line, 3)
        for h in range(2):
            for c in rs_a(w, line, h):
                c.wait_recv()
            o[a, h, i, :, 0:1024] = fsum(o[a, h, i, :, 0:1024], ra[n, h, 0])
            o[b, h, k, :, 1024:2048] = fsum(o[b, h, k, :, 1024:2048], ra[n, h, 1])
            for c in rs_b(w, line, h):
                c.start()

    def st_rc(w, line):
        n = 4 * w + line
        a, i = unit(w, line, 0)
        for h in range(2):
            for c in rs_b(w, line, h):
                c.wait_recv()
            o[a, h, i] = fsum(o[a, h, i], rb[n, h, 0], rb[n, h, 1])

    def forward(w, h):
        plus, minus = passed[w][h]
        return (
            rcopy(pa.at[w, h, 0], pg.at[w, h, 0], rs_s.at[2], pg_r.at[w, h, 0], plus),
            rcopy(pa.at[w, h, 1], pg.at[w, h, 1], rs_s.at[2], pg_r.at[w, h, 1], minus),
        )

    def st_forward(w):
        for h in range(2):
            for side in range(2):
                rs_c(w, h)[side].wait_recv()
                forward(w, h)[side].start()

    def side_sums(w, h):
        for side in range(2):
            for c in rs_d(side)(w, h):
                c.wait_recv()

    def other_plane(h):
        s = SLOT[1][0]
        side_sums(1, h)
        o[s, h, 0] = fsum(o[s, h, 0], pd[1, h, 0], pd[1, h, 1])
        rsz(h).start()

    def result(h):
        s = SLOT[0][0]
        side_sums(0, h)
        rsz(h).wait_recv()
        for w in range(2):
            for c in forward(w, h):
                c.wait_recv()
        for k in range(2):
            c = slice(k * 1024, k * 1024 + 1024)
            out[h * 16 : (h + 1) * 16, c] = fsum(
                o[s, h, 0, :, c], pd[0, h, 0, :, c], pd[0, h, 1, :, c], rz[h, :, c], pg[0, h, k], pg[1, h, k]
            )

    def body(i, carry):
        def on(n, *fns):
            @pl.when(i == n)
            def _():
                for f in fns:
                    f()

        @pl.when(i >= 1)
        def _():
            st_e1(i - 1)

        on(1, ev_rescale_down, lambda: ev_p2(1, (0,)), ev_f1w1)
        on(2, lambda: ev_p2(1, (1, 3)))
        on(3, lambda: ev_p2(1, (2,)))
        on(4, lambda: ev_f2(1), lambda: ev_p2(0, (2,)))
        on(5, lambda: ev_f2(0))
        st_g(i)
        on(0, ev_p1w1)
        on(1, lambda: start(ag_p2((1, 3, 2)), 0), lambda: st_e2(0))
        on(2, lambda: ev_p2(0, (0,)))

        @pl.when(i >= 4)
        def _():
            st_d(i - 4)

        on(4, lambda: st_ra(0, 0))
        on(5, lambda: st_ra(1, 0), lambda: st_rb(0, 0))
        on(6, lambda: st_rb(1, 0))
        on(7, lambda: st_ra(1, 1), lambda: st_ra(1, 3))

        @pl.when(i >= 3)
        def _():
            st_e2(i - 2)

        @pl.when(i >= 3)
        def _():
            st_e3(i - 3)

        on(3, lambda: ev_p2(0, (1, 3)))
        on(6, lambda: st_rc(0, 0))
        on(7, lambda: st_rc(1, 0))
        return carry

    lax.fori_loop(0, NCHUNK, body, 0)

    st_e1(7)
    st_e2(6)
    st_d(4)
    st_ra(1, 2)
    st_rb(1, 1)
    st_rb(1, 3)
    st_e3(5)
    for k, ref in enumerate((x.at[0], x.at[0, 0], x.at[pl.ds(0, 4)], x.at[pl.ds(0, 2)], x.at[0, 0, pl.ds(0, 2)])):
        all_of(ref, ag_s.at[k])
    for k, ref in enumerate((sg, su, sd)):
        all_of(ref.at[pl.ds(0, 8)], sc_s.at[k])
    st_d(5)
    st_ra(0, 2)
    st_e2(7)
    st_rb(1, 2)
    st_e3(6)
    st_rc(1, 1)
    start(rs_d(0), 1)
    st_rc(1, 3)
    start(rs_d(1), 1)
    st_d(6)
    st_ra(0, 1)
    st_ra(0, 3)
    st_rb(0, 2)
    st_e3(7)
    st_rc(1, 2)
    start(rs_c, 1)
    st_d(7)
    st_rb(0, 1)
    st_rb(0, 3)
    st_rc(0, 2)
    start(rs_c, 0)
    for h in range(2):
        other_plane(h)
    st_forward(1)
    st_rc(0, 1)
    start(rs_d(0), 0)
    st_rc(0, 3)
    start(rs_d(1), 0)
    st_forward(0)
    for k, ref in enumerate((r1, r2, hid.at[pl.ds(0, 2)], hid.at[pl.ds(0, 4)])):
        all_of(ref, ch_s.at[k])
    for k, ref in enumerate((x.at[pl.ds(0, 2)], x.at[pl.ds(0, 4)], x.at[0], x.at[0], rz)):
        all_of(ref, rs_s.at[k])
    for h in range(2):
        result(h)


def per_device(tokens, gate_codes, up_codes, down_codes, gate_scales, up_scales, down_scales):
    anyspace = pl.BlockSpec(memory_space=pl.ANY)
    dma = pltpu.SemaphoreType.DMA
    V = pltpu.VMEM
    return pl.pallas_call(
        kernel,
        name="ffn",
        out_shape=pltpu.VMEM((32, 2048), BF),
        in_specs=[anyspace] * 7,
        out_specs=pl.BlockSpec(memory_space=pltpu.VMEM),
        scratch_shapes=[
            V((8, 2, 4, 16, 2048), BF),
            V((8, 2, 4, 16, 2048), BF),
            V((2048, 1792), BF),
            V((896, 2048), BF),
            V((256, 896), I32),
            V((256, 896), I32),
            V((112, 2048), I32),
            V((32, 2048), BF),
            V((2, 28672), BF),
            V((2, 28672), BF),
            V((224, 256), BF),
            V((232, 256), F32),
            V((33, 8, 256), F32),
            V((9, 2, 896), BF),
            V((9, 2, 896), BF),
            V((24, 896), F32),
            V((24, 896), F32),
            V((16, 2048), F32),
            V((8, 2, 2, 32, 1792), BF),
            V((8, 2, 32, 1792), BF),
            V((8, 32, 1792), BF),
            V((8, 32, 1792), BF),
            V((8, 2, 2, 32, 896), BF),
            V((8, 2, 2, 16, 1024), BF),
            V((8, 2, 2, 16, 2048), BF),
            V((2, 2, 2, 16, 1024), BF),
            V((2, 2, 2, 16, 1024), BF),
            V((2, 2, 2, 16, 2048), BF),
            V((2, 16, 2048), BF),
            dma((7,)),
            dma((3,)), dma((3,)),
            dma((5,)), dma((2, 2, 18)), dma((2,)),
            dma((4,)), dma((8,)), dma((8,)), dma((8,)), dma((8,)),
            dma((5,)), dma((8, 2, 2)), dma((8, 2, 2)), dma((2, 2, 2)), dma((2, 2, 2)), dma((2, 2, 2)), dma((2,)),
        ],
        compiler_params=pltpu.CompilerParams(
            collective_id=0, has_side_effects=True, vmem_limit_bytes=60 * 1024 * 1024
        ),
    )(tokens, gate_codes, up_codes, down_codes, gate_scales, up_scales, down_scales.T)


def solution(mesh):
    return jax.shard_map(
        per_device,
        mesh=mesh,
        in_specs=(
            P("row", "col"),
            P("col", "row"),
            P("col", "row"),
            P("row", "col"),
            P("row", None),
            P("row", None),
            P("row", None),
        ),
        out_specs=P("row", "col"),
        check_vma=False,
    )
```
